32 devices in a mesh: row: 4 (over y, core), col: 8 (over z, x).
Axes of the slice: x: 2, y: 2, z: 4, core: 2. Of those that a mesh axis runs over, the one named last changes fastest.
Arguments:
- phases: int32 [4, 8, 8, 24, 576], P('row', 'col'), may hold values from 0 to 2
- grain: float32 [4, 8, 8, 24, 576], P('row', 'col'), may hold values from 0.5 to 2
- phase_cond: float32 [3], replicated, may hold values from 0.3 to 3
- micro_counts: int32 [4, 8, 8], P('row', 'col'), may hold values from 6 to 12, as said below
- current: float32 [4, 8, 8], P('row', 'col'), may hold values from -5 to 5
- load: float32 [4, 8, 8], P('row', 'col'), may hold values from -16 to 16
Outputs:
- states: float32 [4, 8, 8, 3, 24, 576], P('row', 'col')
- tangent: float32 [4, 8, 8, 3, 3], P('row', 'col')
- increment: float32 [4, 8, 8], P('row', 'col')
- residual: float32 [4, 8, 8], P('row', 'col')
The draws below stay inside these ranges and needn't reach their ends.
Inputs may be any that keep to these rules, and one draw needn't show every extreme that they name: `micro_counts`: every draw has an element with 12 inner iterations and one with 6.
All inputs are finite; a program needn't handle non-finite values.
Results may differ from the reference program's by a relative error of at most 0.0003.
Values sent between devices are 32-bit elements; how exact they have to be, the bound alone decides.
A program may use at most 64 MiB of HBM per device.

```python
import math
import jax
import jax.numpy as jnp
from jax import lax

VOX = 24
YZ = 576
PHASES = 3
EZ = 8
MICRO_MAX = 12
MICRO_MIN = 6
MACRO_ITERS = 8
NEX = 4
NEY = 8


def draw_micro_counts(key, part):
    first_key, second_key = jax.random.split(jax.random.fold_in(key, 11))
    base = jax.random.randint(first_key, (NEX, NEY, 1), MICRO_MIN, MICRO_MAX + 1)
    jitter = jax.random.randint(second_key, (NEX, NEY, EZ), -1, 2)
    counts = jnp.clip(base + jitter, MICRO_MIN, MICRO_MAX)
    counts = counts.at[0, 0, 0].set(MICRO_MAX).at[0, 0, 1].set(MICRO_MIN)
    return counts.astype(jnp.int32)


def draw_load(key, part):
    along_x = jnp.arange(NEX, dtype=jnp.float32)[:, None, None] / (NEX - 1)
    along_y = jnp.arange(NEY, dtype=jnp.float32)[None, :, None] / (NEY - 1)
    scale = (1.0 + along_x) * (1.0 + along_y)
    sub_key = jax.random.fold_in(key, 23)
    values = jnp.clip(jax.random.normal(sub_key, (NEX, NEY, EZ), jnp.float32), -4.0, 4.0)
    return (scale * values).astype(jnp.float32)


def plant(entries, own_key, least, high):
    spot = [jax.random.randint(jax.random.fold_in(own_key, axis), (), 0, length) for axis, length in enumerate(entries.shape)]
    longest = entries.shape.index(max(entries.shape))
    next_to = spot[:longest] + [(spot[longest] + 1) % entries.shape[longest]] + spot[longest + 1:]
    return entries.at[tuple(spot)].set(least).at[tuple(next_to)].set(high)


def block_levels(stream_key, extent, shards, least, top_value):
    def one(position, shards_of):
        heights = jax.random.uniform(jax.random.fold_in(jax.random.fold_in(stream_key, 6), position), (shards_of,), jnp.float32, least / len(shards), top_value / len(shards))
        return jnp.repeat(jnp.exp(heights), extent[position] // shards_of).reshape((-1,) + (1,) * (len(extent) - position - 1))

    loudness = one(*shards[0])
    for cut in shards[1:]:
        loudness = loudness * one(*cut)
    return loudness


def noise(rng, shape, deviation, most, cuts=(), kind=jnp.bfloat16):
    gain = block_levels(rng, shape, cuts, -0.22, 0.18) if cuts else 1.0
    entries = jax.random.normal(rng, shape, jnp.float32) * deviation * gain
    return jnp.minimum(jnp.maximum(entries, -most), most).astype(kind)


def setup_inputs(seed: int = 0) -> dict:
    seeds = jax.random.split(jax.random.key(seed), 7)
    phases = plant(jax.random.randint(seeds[0], (NEX, NEY, EZ, VOX, YZ), 0, PHASES), jax.random.fold_in(seeds[0], 1), 0, PHASES - 1).astype(jnp.int32)
    grain = jnp.clip(jnp.exp(math.log(2.0) - 1.3862944 * jax.random.uniform(seeds[1], (NEX, NEY, EZ, VOX, YZ), jnp.float32) ** block_levels(seeds[1], (NEX, NEY, EZ, VOX, YZ), ((0, 4), (1, 8)), -0.2, 0.2)), 0.5, 2.0)
    phase_cond = jnp.clip(jnp.exp(jax.random.uniform(seeds[2], (PHASES,), jnp.float32, math.log(0.3), math.log(3.0))), 0.3, 3.0)
    micro_counts = draw_micro_counts(jax.random.fold_in(seeds[6], 71), 0)
    current = noise(seeds[4], (NEX, NEY, EZ), 1.0, 5.0, ((0, 4), (1, 8)), jnp.float32)
    load = draw_load(jax.random.fold_in(seeds[6], 71), 0)
    return {"phases": phases, "grain": grain, "phase_cond": phase_cond, "micro_counts": micro_counts, "current": current, "load": load}


def forward(field, axis_id):
    z_index = jnp.arange(YZ) % VOX
    if axis_id == 0:
        return jnp.roll(field, -1, axis=-2)
    if axis_id == 1:
        return jnp.roll(field, -VOX, axis=-1)
    return jnp.where(z_index == VOX - 1, jnp.roll(field, VOX - 1, axis=-1), jnp.roll(field, -1, axis=-1))


def behind(field, axis_id):
    z_index = jnp.arange(YZ) % VOX
    if axis_id == 0:
        return jnp.roll(field, 1, axis=-2)
    if axis_id == 1:
        return jnp.roll(field, VOX, axis=-1)
    return jnp.where(z_index == 0, jnp.roll(field, 1 - VOX, axis=-1), jnp.roll(field, 1, axis=-1))


def solve_rve(conduct, count):
    faces = [(conduct + forward(conduct, axis_id)) * 0.5 for axis_id in range(3)]
    back_faces = [behind(faces[axis_id], axis_id) for axis_id in range(3)]
    rhs = jnp.stack([faces[axis_id] - back_faces[axis_id] for axis_id in range(3)])

    def operate(field):
        total = jnp.zeros_like(field)
        for axis_id in range(3):
            total = total + faces[axis_id] * (field - forward(field, axis_id))
            total = total + back_faces[axis_id] * (field - behind(field, axis_id))
        return total

    def sweep(index, carry):
        fluct, remain, direction, norm_now = carry
        image = operate(direction)
        step_size = norm_now / jnp.sum(direction * image, axis=(1, 2))
        fluct = fluct + step_size[:, None, None] * direction
        remain = remain - step_size[:, None, None] * image
        norm_next = jnp.sum(remain * remain, axis=(1, 2))
        direction = remain + (norm_next / norm_now)[:, None, None] * direction
        return fluct, remain, direction, norm_next

    start = (jnp.zeros_like(rhs), rhs, rhs, jnp.sum(rhs * rhs, axis=(1, 2)))
    fluct = lax.fori_loop(0, count, sweep, start)[0]
    identity = jnp.eye(3, dtype=conduct.dtype)
    rows_out = []
    for axis_id in range(3):
        flux = faces[axis_id][None] * (identity[axis_id][:, None, None] + forward(fluct, axis_id) - fluct)
        rows_out.append(jnp.mean(flux, axis=(1, 2)))
    return fluct, jnp.stack(rows_out)


def neighbour(padded, axis_id, offset):
    lead = padded.ndim - 3
    index = [slice(None)] * lead + [slice(1, -1)] * 3
    length = padded.shape[lead + axis_id]
    index[lead + axis_id] = slice(1 + offset, length - 1 + offset)
    return padded[tuple(index)]


def coarse_apply(k_padded, v_padded):
    centre = neighbour(v_padded, 0, 0)
    total = jnp.zeros_like(centre)
    for axis_id in range(3):
        k_centre = neighbour(k_padded[axis_id], 0, 0)
        for offset in (1, -1):
            cond_face = 0.5 * (k_centre + neighbour(k_padded[axis_id], axis_id, offset))
            total = total + cond_face * (centre - neighbour(v_padded, axis_id, offset))
    return total


def reference(phases, grain, phase_cond, micro_counts, current, load):
    conduct = jnp.zeros(grain.shape, grain.dtype)
    for phase_id in range(PHASES):
        conduct = conduct + jnp.where(phases == phase_id, phase_cond[phase_id], 0.0)
    conduct = conduct * grain
    flat = conduct.reshape(-1, VOX, YZ)
    counts = micro_counts.reshape(-1).astype(jnp.int32)
    fluct, tangent = lax.map(lambda pair: solve_rve(pair[0], pair[1]), (flat, counts))
    states = fluct.reshape(NEX, NEY, EZ, 3, VOX, YZ)
    tangent = tangent.reshape(NEX, NEY, EZ, 3, 3)
    diag = jnp.stack([tangent[..., axis_id, axis_id] for axis_id in range(3)])
    k_padded = jnp.pad(diag, ((0, 0), (1, 1), (1, 1), (1, 1)))
    residual = load - coarse_apply(k_padded, jnp.pad(current, 1))
    increment = jnp.zeros_like(residual)
    direction = residual
    norm_now = jnp.sum(residual * residual)
    for iteration in range(MACRO_ITERS):
        image = coarse_apply(k_padded, jnp.pad(direction, 1))
        step_size = norm_now / jnp.sum(direction * image)
        increment = increment + step_size * direction
        residual = residual - step_size * image
        norm_next = jnp.sum(residual * residual)
        direction = residual + (norm_next / norm_now) * direction
        norm_now = norm_next
    return states, tangent, increment, residual
```

```python
import functools

import jax
import jax.numpy as jnp
from jax import lax
from jax.experimental import pallas as pl
from jax.experimental.pallas import tpu as pltpu
from jax.sharding import PartitionSpec as P

VOX = 24
YZ = 576
PHASES = 3
MACRO_ITERS = 8

XC, YC, ZC = 3, 12, 3
ELEMENTS = 8
HALF = YZ // 2
SPANS = ((0, 128), (128, 128), (256, 32))


def swap_half(value):
    lane = lax.broadcasted_iota(jnp.int32, value.shape, 1)
    return jnp.where((lane & 8) == 0, pltpu.roll(value, 120, 1), pltpu.roll(value, 8, 1))


def next_x(value):
    return pltpu.roll(value, 112, 1)


def prev_x(value):
    return pltpu.roll(value, 16, 1)


def next_z(value):
    return pltpu.roll(value, 7, 0)


def prev_z(value):
    return pltpu.roll(value, 1, 0)


def total_of(value):
    for shift in (1, 2, 4):
        value = value + pltpu.roll(value, shift, 0)
    for shift in (8, 16, 32, 64):
        value = value + pltpu.roll(value, shift, 1)
    return value


def cells(pairs):
    return [(xc, zc) for xc in range(XC) for zc in range(ZC)]


SPOTS = cells(None)


def plane(ref, yc, lead=()):
    return {(xc, zc): ref[(*lead, xc, yc, zc)] for xc, zc in SPOTS}


def ahead_x(values, xc, zc):
    return values[xc + 1, zc] if xc < XC - 1 else next_x(values[0, zc])


def back_x(values, xc, zc):
    return values[xc - 1, zc] if xc > 0 else prev_x(values[XC - 1, zc])


def ahead_z(values, xc, zc):
    return values[xc, zc + 1] if zc < ZC - 1 else next_z(values[xc, 0])


def back_z(values, xc, zc):
    return values[xc, zc - 1] if zc > 0 else prev_z(values[xc, ZC - 1])


def swapped(values):
    return {spot: swap_half(value) for spot, value in values.items()}


class Sum:
    def __init__(self, ways=4):
        self.parts = [None] * ways
        self.at = 0

    def add(self, value):
        slot = self.at % len(self.parts)
        self.at += 1
        self.parts[slot] = value if self.parts[slot] is None else self.parts[slot] + value

    def get(self):
        parts = [part for part in self.parts if part is not None]
        while len(parts) > 1:
            parts = [sum(parts[i : i + 2][1:], parts[i]) for i in range(0, len(parts), 2)]
        return parts[0]


def micro_kernel(
    phases_ref, grain_ref, pc_ref, counts_ref, states_ref, tangent_ref,
    rows, turned, cond, faces, rhs, fluct, remain, direction, image, scal,
):
    pc = [pc_ref[k] for k in range(PHASES)]
    for e in range(ELEMENTS):
        phase = phases_ref[e]
        value = jnp.where(phase == 0, pc[0], jnp.where(phase == 1, pc[1], pc[2])) * grain_ref[e]
        for yh in range(2):
            base = (yh * ELEMENTS + e) * VOX
            for t, (start, size) in enumerate(SPANS):
                rows[t, base : base + VOX, 0:size] = value[:, yh * HALF + start : yh * HALF + start + size]
    for xc in range(XC):
        for t, (start, size) in enumerate(SPANS):
            parts = []
            for xs in range(8):
                for yh in range(2):
                    parts.append(rows.at[t][pl.ds(yh * ELEMENTS * VOX + 3 * xs + xc, 8, stride=VOX), :])
            block = jnp.concatenate(parts, axis=0).T
            turned[xc * HALF + start : xc * HALF + start + size, :] = block[0:size]
    for xc in range(XC):
        for yc in range(YC):
            for zc in range(ZC):
                cond[xc, yc, zc] = turned[pl.ds(xc * HALF + yc * VOX + zc, 8, stride=3), :]

    face_sums = [Sum(), Sum(), Sum()]
    here = plane(cond, 0)
    for yc in range(YC):
        ahead = plane(cond, yc + 1) if yc < YC - 1 else swapped(plane(cond, 0))
        for xc, zc in SPOTS:
            own = here[xc, zc]
            for d, other in enumerate((ahead_x(here, xc, zc), ahead[xc, zc], ahead_z(here, xc, zc))):
                face = (own + other) * 0.5
                faces[d, xc, yc, zc] = face
                face_sums[d].add(face)
        here = ahead
    norms = [Sum(), Sum(), Sum()]
    before = swapped(plane(faces, YC - 1, (1,)))
    for yc in range(YC):
        fx, fy, fz = (plane(faces, yc, (d,)) for d in range(3))
        for xc, zc in SPOTS:
            backs = (back_x(fx, xc, zc), before[xc, zc], back_z(fz, xc, zc))
            for d, own in enumerate((fx[xc, zc], fy[xc, zc], fz[xc, zc])):
                value = own - backs[d]
                rhs[d, xc, yc, zc] = value
                remain[d, xc, yc, zc] = value
                norms[d].add(value * value)
        before = fy

    lane = lax.broadcasted_iota(jnp.int32, (8, 128), 1)
    counts = jnp.zeros((8, 128), jnp.int32)
    longest = counts_ref[0]
    for e in range(ELEMENTS):
        counts = jnp.where((lane & 7) == e, counts_ref[e], counts)
        longest = jnp.maximum(longest, counts_ref[e])

    def sweep(c, alpha, beta, first):
        curv = Sum()

        def fresh(yc):
            out = {}
            for xc, zc in SPOTS:
                at = (c, xc, yc, zc)
                if first:
                    value = remain[at]
                    fluct[at] = jnp.zeros((8, 128), jnp.float32)
                else:
                    old = direction[at]
                    fluct[at] = fluct[at] + alpha * old
                    value = remain[at] + beta * old
                direction[at] = value
                out[xc, zc] = value
            return out

        last = fresh(YC - 1)
        here = fresh(0)
        flow_back = {
            s: swap_half(faces[1, s[0], YC - 1, s[1]] * (last[s] - swap_half(here[s]))) for s in SPOTS
        }
        for yc in range(YC):
            if yc < YC - 2:
                ahead = fresh(yc + 1)
            elif yc == YC - 2:
                ahead = plane(direction, YC - 1, (c,))
            else:
                ahead = swapped(plane(direction, 0, (c,)))
            gx, gy, gz = {}, {}, {}
            for xc, zc in SPOTS:
                own = here[xc, zc]
                gx[xc, zc] = faces[0, xc, yc, zc] * (own - ahead_x(here, xc, zc))
                gy[xc, zc] = faces[1, xc, yc, zc] * (own - ahead[xc, zc])
                gz[xc, zc] = faces[2, xc, yc, zc] * (own - ahead_z(here, xc, zc))
            for xc, zc in SPOTS:
                value = (
                    (gx[xc, zc] - back_x(gx, xc, zc))
                    + (gy[xc, zc] - flow_back[xc, zc])
                    + (gz[xc, zc] - back_z(gz, xc, zc))
                )
                image[c, xc, yc, zc] = value
                curv.add(here[xc, zc] * value)
            flow_back = gy
            here = ahead
        return total_of(curv.get())

    def reduce_residual(c, alpha):
        norm = Sum()
        for yc in range(YC):
            for xc, zc in SPOTS:
                at = (c, xc, yc, zc)
                value = remain[at] - alpha * image[at]
                remain[at] = value
                norm.add(value * value)
        return total_of(norm.get())

    for c in range(3):
        norm = total_of(norms[c].get())
        curv = sweep(c, None, None, True)
        scal[0, c] = norm
        scal[1, c] = norm / curv

    def iterate(index, carry):
        for c in range(3):
            alpha = scal[1, c]
            norm = scal[0, c]
            norm_next = reduce_residual(c, alpha)
            curv = sweep(c, alpha, norm_next / norm, False)
            scal[0, c] = norm_next
            scal[1, c] = jnp.where(index < counts, norm_next / curv, 0.0)
        return carry

    lax.fori_loop(1, longest, iterate, 0)

    scale = 1.0 / (VOX * YZ)
    for c in range(3):
        alpha = scal[1, c]
        sums = [Sum(2), Sum(2), Sum(2)]
        for xc in range(XC):
            for yc in range(YC):
                for zc in range(ZC):
                    at = (c, xc, yc, zc)
                    value = fluct[at] + alpha * direction[at]
                    turned[pl.ds(xc * HALF + yc * VOX + zc, 8, stride=3), :] = value
                    for d in range(3):
                        sums[d].add(value * rhs[d, xc, yc, zc])
        for d in range(3):
            entry = -sums[d].get()
            if d == c:
                entry = entry + face_sums[d].get()
            tangent_ref[d * 3 + c] = total_of(entry) * scale
        for xc in range(XC):
            for t, (start, size) in enumerate(SPANS):
                block = turned[xc * HALF + start : xc * HALF + start + size, :].T
                for xs in range(8):
                    for yh in range(2):
                        row = (xs * 2 + yh) * 8
                        piece = block[row : row + 8]
                        if size < 128:
                            piece = jnp.concatenate([piece, jnp.zeros((8, 128 - size), jnp.float32)], axis=1)
                        rows.at[t][pl.ds(yh * ELEMENTS * VOX + 3 * xs + xc, 8, stride=VOX), :] = piece
        for e in range(ELEMENTS):
            for yh in range(2):
                base = (yh * ELEMENTS + e) * VOX
                for t, (start, size) in enumerate(SPANS):
                    states_ref[e, c, :, yh * HALF + start : yh * HALF + start + size] = rows[
                        t, base : base + VOX, 0:size
                    ]


def micro(phases, grain, phase_cond, counts):
    field = pltpu.VMEM((3, XC, YC, ZC, 8, 128), jnp.float32)
    vmem = pl.BlockSpec(memory_space=pltpu.VMEM)
    smem = pl.BlockSpec(memory_space=pltpu.SMEM)
    return pl.pallas_call(
        micro_kernel,
        out_shape=(
            jax.ShapeDtypeStruct((ELEMENTS, 3, VOX, YZ), jnp.float32),
            jax.ShapeDtypeStruct((9, 8, 128), jnp.float32),
        ),
        in_specs=[vmem, vmem, smem, smem],
        out_specs=(vmem, vmem),
        scratch_shapes=[
            pltpu.VMEM((3, 2 * ELEMENTS * VOX, 128), jnp.float32),
            pltpu.VMEM((XC * HALF, 128), jnp.float32),
            pltpu.VMEM((XC, YC, ZC, 8, 128), jnp.float32),
            field, field, field, field, field, field,
            pltpu.VMEM((2, 3, 8, 128), jnp.float32),
        ],
        name="micro",
    )(phases, grain, phase_cond, counts)


def neighbour(padded, axis_id, offset):
    lead = padded.ndim - 3
    index = [slice(None)] * lead + [slice(1, -1)] * 3
    length = padded.shape[lead + axis_id]
    index[lead + axis_id] = slice(1 + offset, length - 1 + offset)
    return padded[tuple(index)]


def coarse_apply(k_padded, v_padded):
    centre = neighbour(v_padded, 0, 0)
    total = jnp.zeros_like(centre)
    for axis_id in range(3):
        k_centre = neighbour(k_padded[axis_id], 0, 0)
        for offset in (1, -1):
            cond_face = 0.5 * (k_centre + neighbour(k_padded[axis_id], axis_id, offset))
            total = total + cond_face * (centre - neighbour(v_padded, axis_id, offset))
    return total


def coarse_cg(k_padded, residual):
    increment = jnp.zeros_like(residual)
    direction = residual
    norm_now = jnp.sum(residual * residual)
    for iteration in range(MACRO_ITERS):
        image = coarse_apply(k_padded, jnp.pad(direction, 1))
        step_size = norm_now / jnp.sum(direction * image)
        increment = increment + step_size * direction
        residual = residual - step_size * image
        norm_next = jnp.sum(residual * residual)
        direction = residual + norm_next / norm_now * direction
        norm_now = norm_next
    return (increment, residual)


def shards(phases, grain, phase_cond, micro_counts, current, load):
    depth = phases.shape[2]
    states, tangents = micro(
        phases.reshape(depth, VOX, YZ), grain.reshape(depth, VOX, YZ), phase_cond, micro_counts.reshape(depth)
    )
    tangent = tangents[:, 0, 0:depth]
    diag = tangent[0:9:4].reshape(3, 1, 1, depth)
    packed = jnp.concatenate(
        [diag, current.reshape(1, 1, 1, depth), load.reshape(1, 1, 1, depth)], axis=0
    ).reshape(5, 1, depth)
    whole = lax.all_gather(packed, ("row", "col"), axis=1, tiled=True)
    whole = whole.reshape(5, lax.axis_size("row"), lax.axis_size("col"), depth)
    padded = jnp.pad(whole, ((0, 0), (1, 1), (1, 1), (1, 1)))
    residual = whole[4] - coarse_apply(padded[:3], padded[3])
    increment, residual = coarse_cg(padded[:3], residual)
    row_at = lax.axis_index("row")
    col_at = lax.axis_index("col")
    zero_at = jnp.zeros((), jnp.int32)
    increment = lax.dynamic_slice(increment, (row_at, col_at, zero_at), (1, 1, depth))
    residual = lax.dynamic_slice(residual, (row_at, col_at, zero_at), (1, 1, depth))
    return (
        states.reshape(1, 1, depth, 3, VOX, YZ),
        tangent.T.reshape(1, 1, depth, 3, 3),
        increment,
        residual,
    )


def solution(mesh):
    placed = (
        P("row", "col", None, None, None),
        P("row", "col", None, None, None),
        P(),
        P("row", "col", None),
        P("row", "col", None),
        P("row", "col", None),
    )
    return jax.shard_map(
        shards,
        mesh=mesh,
        in_specs=placed,
        out_specs=(
            P("row", "col", None, None, None, None),
            P("row", "col", None, None, None),
            P("row", "col", None),
            P("row", "col", None),
        ),
        check_vma=False,
    )
```

```python
import functools

import jax
import jax.numpy as jnp
from jax import lax
from jax.experimental import pallas as pl
from jax.experimental.pallas import tpu as pltpu
from jax.sharding import PartitionSpec as P

VOX = 24
YZ = 576
PHASES = 3
MACRO_ITERS = 8

XC, YC, ZC = 3, 12, 3
ELEMENTS = 8
HALF = YZ // 2
SPANS = ((0, 128), (128, 128), (256, 32))


def swap_half(value):
    lane = lax.broadcasted_iota(jnp.int32, value.shape, 1)
    return jnp.where((lane & 8) == 0, pltpu.roll(value, 120, 1), pltpu.roll(value, 8, 1))


def next_x(value):
    return pltpu.roll(value, 112, 1)


def prev_x(value):
    return pltpu.roll(value, 16, 1)


def next_z(value):
    return pltpu.roll(value, 7, 0)


def prev_z(value):
    return pltpu.roll(value, 1, 0)


def total_of(value):
    for shift in (1, 2, 4):
        value = value + pltpu.roll(value, shift, 0)
    for shift in (8, 16, 32, 64):
        value = value + pltpu.roll(value, shift, 1)
    return value


SPOTS = [(xc, zc) for xc in range(XC) for zc in range(ZC)]


def plane(ref, yc, lead=()):
    return {(xc, zc): ref[(*lead, xc, yc, zc)] for xc, zc in SPOTS}


def ahead_x(values, xc, zc):
    return values[xc + 1, zc] if xc < XC - 1 else next_x(values[0, zc])


def back_x(values, xc, zc):
    return values[xc - 1, zc] if xc > 0 else prev_x(values[XC - 1, zc])


def ahead_z(values, xc, zc):
    return values[xc, zc + 1] if zc < ZC - 1 else next_z(values[xc, 0])


def back_z(values, xc, zc):
    return values[xc, zc - 1] if zc > 0 else prev_z(values[xc, ZC - 1])


def swapped(values):
    return {spot: swap_half(value) for spot, value in values.items()}


class Sum:
    def __init__(self, ways=4):
        self.parts = [None] * ways
        self.at = 0

    def add(self, value):
        slot = self.at % len(self.parts)
        self.at += 1
        self.parts[slot] = value if self.parts[slot] is None else self.parts[slot] + value

    def get(self):
        parts = [part for part in self.parts if part is not None]
        while len(parts) > 1:
            parts = [sum(parts[i : i + 2][1:], parts[i]) for i in range(0, len(parts), 2)]
        return parts[0]


def micro_kernel(
    phases_ref, grain_ref, pc_ref, counts_ref, current_ref, load_ref, states_ref, tangent_ref, mine_ref,
    rows, turned, cond, faces, rhs, fluct, remain, direction, image, scal,
):
    pc = [pc_ref[k] for k in range(PHASES)]
    for e in range(ELEMENTS):
        phase = phases_ref[0, 0, e]
        value = jnp.where(phase == 0, pc[0], jnp.where(phase == 1, pc[1], pc[2])) * grain_ref[0, 0, e]
        for yh in range(2):
            base = (yh * ELEMENTS + e) * VOX
            for t, (start, size) in enumerate(SPANS):
                rows[t, base : base + VOX, 0:size] = value[:, yh * HALF + start : yh * HALF + start + size]
    for xc in range(XC):
        for t, (start, size) in enumerate(SPANS):
            parts = []
            for xs in range(8):
                for yh in range(2):
                    parts.append(rows.at[t][pl.ds(yh * ELEMENTS * VOX + 3 * xs + xc, 8, stride=VOX), :])
            block = jnp.concatenate(parts, axis=0).T
            turned[xc * HALF + start : xc * HALF + start + size, :] = block[0:size]
    for xc in range(XC):
        for yc in range(YC):
            for zc in range(ZC):
                cond[xc, yc, zc] = turned[pl.ds(xc * HALF + yc * VOX + zc, 8, stride=3), :]

    face_sums = [Sum(), Sum(), Sum()]
    here = plane(cond, 0)
    for yc in range(YC):
        ahead = plane(cond, yc + 1) if yc < YC - 1 else swapped(plane(cond, 0))
        for xc, zc in SPOTS:
            own = here[xc, zc]
            for d, other in enumerate((ahead_x(here, xc, zc), ahead[xc, zc], ahead_z(here, xc, zc))):
                face = (own + other) * 0.5
                faces[d, xc, yc, zc] = face
                face_sums[d].add(face)
        here = ahead
    norms = [Sum(), Sum(), Sum()]
    before = swapped(plane(faces, YC - 1, (1,)))
    for yc in range(YC):
        fx, fy, fz = (plane(faces, yc, (d,)) for d in range(3))
        for xc, zc in SPOTS:
            backs = (back_x(fx, xc, zc), before[xc, zc], back_z(fz, xc, zc))
            for d, own in enumerate((fx[xc, zc], fy[xc, zc], fz[xc, zc])):
                value = own - backs[d]
                rhs[d, xc, yc, zc] = value
                remain[d, xc, yc, zc] = value
                norms[d].add(value * value)
        before = fy

    lane = lax.broadcasted_iota(jnp.int32, (8, 128), 1)
    counts = jnp.zeros((8, 128), jnp.int32)
    longest = counts_ref[0, 0, 0]
    for e in range(ELEMENTS):
        counts = jnp.where((lane & 7) == e, counts_ref[0, 0, e], counts)
        longest = jnp.maximum(longest, counts_ref[0, 0, e])

    def sweep(c, alpha, beta, first):
        curv = Sum()

        def fresh(yc):
            out = {}
            for xc, zc in SPOTS:
                at = (c, xc, yc, zc)
                if first:
                    value = remain[at]
                    fluct[at] = jnp.zeros((8, 128), jnp.float32)
                else:
                    old = direction[at]
                    fluct[at] = fluct[at] + alpha * old
                    value = remain[at] + beta * old
                direction[at] = value
                out[xc, zc] = value
            return out

        last = fresh(YC - 1)
        here = fresh(0)
        flow_back = {
            s: swap_half(faces[1, s[0], YC - 1, s[1]] * (last[s] - swap_half(here[s]))) for s in SPOTS
        }
        for yc in range(YC):
            if yc < YC - 2:
                ahead = fresh(yc + 1)
            elif yc == YC - 2:
                ahead = plane(direction, YC - 1, (c,))
            else:
                ahead = swapped(plane(direction, 0, (c,)))
            gx, gy, gz = {}, {}, {}
            for xc, zc in SPOTS:
                own = here[xc, zc]
                gx[xc, zc] = faces[0, xc, yc, zc] * (own - ahead_x(here, xc, zc))
                gy[xc, zc] = faces[1, xc, yc, zc] * (own - ahead[xc, zc])
                gz[xc, zc] = faces[2, xc, yc, zc] * (own - ahead_z(here, xc, zc))
            for xc, zc in SPOTS:
                value = (
                    (gx[xc, zc] - back_x(gx, xc, zc))
                    + (gy[xc, zc] - flow_back[xc, zc])
                    + (gz[xc, zc] - back_z(gz, xc, zc))
                )
                image[c, xc, yc, zc] = value
                curv.add(here[xc, zc] * value)
            flow_back = gy
            here = ahead
        return total_of(curv.get())

    def reduce_residual(c, alpha):
        norm = Sum()
        for yc in range(YC):
            for xc, zc in SPOTS:
                at = (c, xc, yc, zc)
                value = remain[at] - alpha * image[at]
                remain[at] = value
                norm.add(value * value)
        return total_of(norm.get())

    for c in range(3):
        norm = total_of(norms[c].get())
        curv = sweep(c, None, None, True)
        scal[0, c] = norm
        scal[1, c] = norm / curv

    def iterate(index, carry):
        for c in range(3):
            alpha = scal[1, c]
            norm = scal[0, c]
            norm_next = reduce_residual(c, alpha)
            curv = sweep(c, alpha, norm_next / norm, False)
            scal[0, c] = norm_next
            scal[1, c] = jnp.where(index < counts, norm_next / curv, 0.0)
        return carry

    lax.fori_loop(1, longest, iterate, 0)

    scale = 1.0 / (VOX * YZ)
    entries = {}
    for c in range(3):
        alpha = scal[1, c]
        sums = [Sum(2), Sum(2), Sum(2)]
        for xc in range(XC):
            for yc in range(YC):
                for zc in range(ZC):
                    at = (c, xc, yc, zc)
                    value = fluct[at] + alpha * direction[at]
                    turned[pl.ds(xc * HALF + yc * VOX + zc, 8, stride=3), :] = value
                    for d in range(3):
                        sums[d].add(value * rhs[d, xc, yc, zc])
        for d in range(3):
            entry = -sums[d].get()
            if d == c:
                entry = entry + face_sums[d].get()
            entries[d, c] = total_of(entry) * scale
        for xc in range(XC):
            for t, (start, size) in enumerate(SPANS):
                block = turned[xc * HALF + start : xc * HALF + start + size, :].T
                for xs in range(8):
                    for yh in range(2):
                        row = (xs * 2 + yh) * 8
                        piece = block[row : row + 8]
                        if size < 128:
                            piece = jnp.concatenate([piece, jnp.zeros((8, 128 - size), jnp.float32)], axis=1)
                        rows.at[t][pl.ds(yh * ELEMENTS * VOX + 3 * xs + xc, 8, stride=VOX), :] = piece
        for e in range(ELEMENTS):
            for yh in range(2):
                base = (yh * ELEMENTS + e) * VOX
                for t, (start, size) in enumerate(SPANS):
                    states_ref[0, 0, e, c, :, yh * HALF + start : yh * HALF + start + size] = rows[
                        t, base : base + VOX, 0:size
                    ]


    row = lax.broadcasted_iota(jnp.int32, (8, 128), 0)
    for d in range(3):
        block = entries[d, 0]
        for c in range(1, 3):
            block = jnp.where(row == c, entries[d, c], block)
        tangent_ref[0, 0, :, d, :] = block.T[0:ELEMENTS, 0:3]
    mine = jnp.where(lane < 8, entries[0, 0], jnp.where(lane < 16, entries[1, 1], entries[2, 2]))
    for e in range(ELEMENTS):
        mine = jnp.where(lane == 3 * ELEMENTS + e, current_ref[0, 0, e], mine)
        mine = jnp.where(lane == 4 * ELEMENTS + e, load_ref[0, 0, e], mine)
    mine_ref[...] = mine[0:1]


def micro(phases, grain, phase_cond, counts, current, load):
    field = pltpu.VMEM((3, XC, YC, ZC, 8, 128), jnp.float32)
    vmem = pl.BlockSpec(memory_space=pltpu.VMEM)
    smem = pl.BlockSpec(memory_space=pltpu.SMEM)
    return pl.pallas_call(
        micro_kernel,
        out_shape=(
            jax.ShapeDtypeStruct((1, 1, ELEMENTS, 3, VOX, YZ), jnp.float32),
            jax.ShapeDtypeStruct((1, 1, ELEMENTS, 3, 3), jnp.float32),
            jax.ShapeDtypeStruct((1, 128), jnp.float32),
        ),
        in_specs=[vmem, vmem, smem, smem, smem, smem],
        out_specs=(vmem, vmem, vmem),
        scratch_shapes=[
            pltpu.VMEM((3, 2 * ELEMENTS * VOX, 128), jnp.float32),
            pltpu.VMEM((XC * HALF, 128), jnp.float32),
            pltpu.VMEM((XC, YC, ZC, 8, 128), jnp.float32),
            field, field, field, field, field, field,
            pltpu.VMEM((2, 3, 8, 128), jnp.float32),
        ],
        name="micro",
    )(phases, grain, phase_cond, counts, current, load)


def macro_kernel(nrow, ncol, depth, mine_ref, inc_ref, res_ref, got, picked, own_sem, send_sems, recv_sems):
    n = nrow * ncol
    me = lax.axis_index("row") * ncol + lax.axis_index("col")

    def peer(k):
        other = lax.rem(me + k, n)
        return {"row": other // ncol, "col": lax.rem(other, ncol)}

    barrier = pltpu.get_barrier_semaphore()

    def greet(k, carry):
        pl.semaphore_signal(barrier, inc=1, device_id=peer(k), device_id_type=pl.DeviceIdType.MESH)
        return carry

    lax.fori_loop(1, n, greet, 0)
    own = pltpu.make_async_copy(mine_ref, got.at[me], own_sem)
    own.start()
    pl.semaphore_wait(barrier, n - 1)

    def copy(k):
        return pltpu.make_async_remote_copy(
            src_ref=mine_ref,
            dst_ref=got.at[me],
            send_sem=send_sems.at[k],
            recv_sem=recv_sems.at[k],
            device_id=peer(k),
            device_id_type=pl.DeviceIdType.MESH,
        )

    def send(k, carry):
        copy(k).start()
        return carry

    def finish(k, carry):
        copy(k).wait()
        return carry

    lax.fori_loop(1, n, send, 0)
    own.wait()
    lax.fori_loop(1, n, finish, 0)

    table = got[...].reshape(n, 128)
    lane = lax.broadcasted_iota(jnp.int32, (n, 128), 1)
    device = lax.broadcasted_iota(jnp.int32, (n, 128), 0)
    inside = lane < depth

    def field(q):
        value = table if q == 0 else pltpu.roll(table, 128 - q * depth, 1)
        return jnp.where(inside, value, 0.0)

    row_at, col_at = device // ncol, lax.rem(device, ncol)
    steps = (
        (0, ncol, row_at < nrow - 1), (0, -ncol, row_at > 0),
        (0, 1, col_at < ncol - 1), (0, -1, col_at > 0),
        (1, 1, lane < depth - 1), (1, -1, lane > 0),
    )

    def shifted(value, axis, step):
        length = n if axis == 0 else 128
        return pltpu.roll(value, (-step) % length, axis)

    weights = []
    centre = jnp.zeros((n, 128), jnp.float32)
    for index, (axis, step, has) in enumerate(steps):
        k = field(index // 2)
        pair = 0.5 * (k + jnp.where(has, shifted(k, axis, step), 0.0))
        centre = centre + pair
        weights.append(jnp.where(has & inside, pair, 0.0))
    centre = jnp.where(inside, centre, 0.0)

    def apply(value):
        parts = [weight * shifted(value, axis, step) for weight, (axis, step, _) in zip(weights, steps)]
        return centre * value - ((parts[0] + parts[1]) + (parts[2] + parts[3]) + (parts[4] + parts[5]))

    def total(value):
        value = jnp.sum(value.reshape(n // 8, 8, 128), axis=0)
        for shift in (1, 2, 4):
            value = value + pltpu.roll(value, shift, 0)
        return jnp.sum(value, axis=1, keepdims=True)[0:1]

    residual = field(4) - apply(field(3))
    increment = jnp.zeros((n, 128), jnp.float32)
    direction = residual
    norm = total(residual * residual)
    for _ in range(MACRO_ITERS):
        image = apply(direction)
        step_size = norm / total(direction * image)
        increment = increment + step_size * direction
        residual = residual - step_size * image
        norm_next = total(residual * residual)
        direction = residual + (norm_next / norm) * direction
        norm = norm_next
    picked[0] = increment
    picked[1] = residual
    inc_ref[0] = picked[0, pl.ds(me, 1), 0:depth]
    res_ref[0] = picked[1, pl.ds(me, 1), 0:depth]


def macro(mine, nrow, ncol, depth):
    n = nrow * ncol
    vmem = pl.BlockSpec(memory_space=pltpu.VMEM)
    small = jax.ShapeDtypeStruct((1, 1, depth), jnp.float32)
    return pl.pallas_call(
        functools.partial(macro_kernel, nrow, ncol, depth),
        out_shape=(small, small),
        in_specs=[vmem],
        out_specs=(vmem, vmem),
        scratch_shapes=[
            pltpu.VMEM((n, 1, 128), jnp.float32),
            pltpu.VMEM((2, n, 128), jnp.float32),
            pltpu.SemaphoreType.DMA,
            pltpu.SemaphoreType.DMA((n,)),
            pltpu.SemaphoreType.DMA((n,)),
        ],
        compiler_params=pltpu.CompilerParams(collective_id=0, has_side_effects=True),
        name="macro",
    )(mine)


def shards(nrow, ncol, phases, grain, phase_cond, micro_counts, current, load):
    depth = phases.shape[2]
    states, tangent, mine = micro(phases, grain, phase_cond, micro_counts, current, load)
    increment, residual = macro(mine, nrow, ncol, depth)
    return (states, tangent, increment, residual)


def solution(mesh):
    placed = (
        P("row", "col", None, None, None),
        P("row", "col", None, None, None),
        P(),
        P("row", "col", None),
        P("row", "col", None),
        P("row", "col", None),
    )
    return jax.shard_map(
        functools.partial(shards, mesh.shape["row"], mesh.shape["col"]),
        mesh=mesh,
        in_specs=placed,
        out_specs=(
            P("row", "col", None, None, None, None),
            P("row", "col", None, None, None),
            P("row", "col", None),
            P("row", "col", None),
        ),
        check_vma=False,
    )
```
